128 devices in a mesh: ctx: 8 (over y_hi, z), fsdp: 16 (over x, y_lo, core).
Axes of the slice: x: 4, y: 4 (y_hi: 2, y_lo: 2; y = y_hi * 2 + y_lo), z: 4, core: 2. Of those that a mesh axis runs over, the one named last changes fastest.
Arguments:
- clean: bfloat16 [4096, 5120], P(('ctx', 'fsdp')), may hold values from -6 to 6
- noise: bfloat16 [4096, 5120], P(('ctx', 'fsdp')), may hold values from -6 to 6
- noise_two: bfloat16 [4096, 5120], P(('ctx', 'fsdp')), may hold values from -6 to 6
- steps_gen: int32 [3], replicated, may hold values from 600 to 959
- steps_teacher: int32 [3], replicated, may hold values from 20 to 979
- cache_key: bfloat16 [2048, 4096], P('ctx', 'fsdp'), may hold values from -6 to 6
- cache_value: bfloat16 [2048, 4096], P('ctx', 'fsdp'), may hold values from -6 to 6
- cache_block: int32 [2048], P('ctx'), may hold values from 0 to 6
- span_block: int32 [1], replicated, may hold values from 2 to 6
- gen_query: bfloat16 [5120, 4096], P(None, 'fsdp'), may hold values from -0.07614237 to 0.07614237
- gen_key: bfloat16 [5120, 4096], P(None, 'fsdp'), may hold values from -0.052146567 to 0.052146567
- gen_value: bfloat16 [5120, 4096], P(None, 'fsdp'), may hold values from -0.078125 to 0.078125
- gen_out: bfloat16 [4096, 5120], P('fsdp'), may hold values from -0.375 to 0.375
- teacher_query: bfloat16 [5120, 4096], P(None, 'fsdp'), may hold values from -0.07614237 to 0.07614237
- teacher_key: bfloat16 [5120, 4096], P(None, 'fsdp'), may hold values from -0.052146567 to 0.052146567
- teacher_value: bfloat16 [5120, 4096], P(None, 'fsdp'), may hold values from -0.078125 to 0.078125
- teacher_out: bfloat16 [4096, 5120], P('fsdp'), may hold values from -0.375 to 0.375
Outputs:
- generated: bfloat16 [4096, 5120], P(('ctx', 'fsdp'))
- grad_out: bfloat16 [4096, 5120], P('fsdp')
The draws below stay inside these ranges and needn't reach their ends.
Inputs may be any that keep to these rules, and one draw needn't show every extreme that they name: span_block holds one id.
All inputs are finite; a program needn't handle non-finite values.
Results may differ from the reference program's by a relative error of at most 0.018.
The reference program's roundings to bfloat16 on the way count: a program that leaves them out, or rounds other values in their place, can miss the bound.
Values may be sent and summed in bfloat16 or wider, within the bound.
No kernel may reach another device: no remote copies, remote signals or barrier semaphores. Data moves between devices by JAX's collectives and lax.ppermute only.
A program may use at most 128 MiB of HBM per device.

```python
import jax
import jax.numpy as jnp
from jax import lax

D = 5120
HEADS = 32
HEAD = 128
FRAMES = 3
STEPS = 1000
NBLK = 7
TOKENS = 4096
CACHE = 2048
INNER = 4096
N_FSDP = 16


def drawn_pair(key, query_scale):
    streams = jax.random.split(key, 5)
    query_base = jax.random.uniform(streams[0], (D, INNER), jnp.float32, -1.7, 1.7)
    key_base = jax.random.uniform(streams[1], (D, INNER), jnp.float32, -1.7, 1.7)
    feature_signs = jax.random.randint(streams[2], (D,), 0, 2).astype(jnp.float32) * 2.0 - 1.0
    head_signs = jax.random.randint(streams[3], (HEADS, HEAD), 0, 2).astype(jnp.float32) * 2.0 - 1.0
    shuffled = jax.random.permutation(streams[4], HEADS)
    aligned_count = max(HEADS // 8, 1)
    picked = (shuffled < aligned_count).astype(jnp.float32)
    amplitude = picked * 0.0
    direction = (amplitude[:, None] * head_signs / HEAD ** 0.5).reshape(INNER)
    outer_part = (feature_signs / D ** 0.5)[:, None] * direction[None, :]
    first = query_base * (query_scale / D ** 0.5) + outer_part
    second = key_base / D ** 0.5 + outer_part
    return (first, second)


def draw_gen_query(key, part):
    return drawn_pair(jax.random.fold_in(key, 11), 2.0)[0].astype(jnp.bfloat16)


def draw_gen_key(key, part):
    return drawn_pair(jax.random.fold_in(key, 11), 2.0)[1].astype(jnp.bfloat16)


def draw_teacher_query(key, part):
    return drawn_pair(jax.random.fold_in(key, 23), 2.0)[0].astype(jnp.bfloat16)


def draw_teacher_key(key, part):
    return drawn_pair(jax.random.fold_in(key, 23), 2.0)[1].astype(jnp.bfloat16)


def set_ends(drawn, rng, least, top_value):
    index_at = [jax.random.randint(jax.random.fold_in(rng, axis), (), 0, length) for axis, length in enumerate(drawn.shape)]
    longest = drawn.shape.index(max(drawn.shape))
    next_to = index_at[:longest] + [(index_at[longest] + 1) % drawn.shape[longest]] + index_at[longest + 1:]
    return drawn.at[tuple(index_at)].set(least).at[tuple(next_to)].set(top_value)


def levels(rng, shape, cuts, smallest, high):
    level = 1.0
    for axis_at, shards_of in cuts:
        draws = jax.random.uniform(jax.random.fold_in(jax.random.fold_in(rng, 6), axis_at), (shards_of,), jnp.float32, smallest / len(cuts), high / len(cuts))
        level = level * jnp.repeat(jnp.exp(draws), shape[axis_at] // shards_of).reshape((-1,) + (1,) * (len(shape) - 1 - axis_at))
    return level


def scatter_about(rng, shape, scale, limit, cuts=(), held_as=jnp.bfloat16):
    array = scale * jax.random.normal(rng, shape, jnp.float32)
    if cuts:
        array = array * levels(rng, shape, cuts, -0.22, 0.18)
    return jnp.clip(array, -limit, limit).astype(held_as)


def setup_inputs(seed: int = 0) -> dict:
    seeds = jax.random.split(jax.random.key(seed), 18)
    clean = scatter_about(seeds[0], (TOKENS, D), 1.0, 6.0, ((0, 128),))
    noise = scatter_about(seeds[1], (TOKENS, D), 1.0, 6.0, ((0, 128),))
    noise_two = scatter_about(seeds[2], (TOKENS, D), 1.0, 6.0, ((0, 128),))
    steps_gen = jax.random.randint(seeds[3], (FRAMES,), 600, 960).astype(jnp.int32)
    steps_teacher = jax.random.randint(seeds[4], (FRAMES,), 20, 980).astype(jnp.int32)
    cache_key = scatter_about(seeds[5], (CACHE, INNER), 1.0, 6.0, ((0, 8), (1, 16)))
    cache_value = scatter_about(seeds[6], (CACHE, INNER), 1.0, 6.0, ((0, 8), (1, 16)))
    cache_block = set_ends(jax.random.randint(seeds[7], (CACHE,), 0, NBLK), jax.random.fold_in(seeds[7], 1), 0, NBLK - 1).astype(jnp.int32)
    span_block = jax.random.randint(seeds[8], (1,), 2, NBLK).astype(jnp.int32)
    gen_query = draw_gen_query(jax.random.fold_in(seeds[17], 71), 0)
    gen_key = draw_gen_key(jax.random.fold_in(seeds[17], 71), 0)
    gen_value = scatter_about(seeds[11], (D, INNER), D ** -0.5, 0.078125, ((1, 16),))
    gen_out = scatter_about(seeds[12], (INNER, D), (INNER // 16) ** -0.5, 0.375, ((0, 16),))
    teacher_query = draw_teacher_query(jax.random.fold_in(seeds[17], 71), 0)
    teacher_key = draw_teacher_key(jax.random.fold_in(seeds[17], 71), 0)
    teacher_value = scatter_about(seeds[15], (D, INNER), D ** -0.5, 0.078125, ((1, 16),))
    teacher_out = scatter_about(seeds[16], (INNER, D), (INNER // 16) ** -0.5, 0.375, ((0, 16),))
    return {"clean": clean, "noise": noise, "noise_two": noise_two, "steps_gen": steps_gen, "steps_teacher": steps_teacher, "cache_key": cache_key, "cache_value": cache_value, "cache_block": cache_block, "span_block": span_block, "gen_query": gen_query, "gen_key": gen_key, "gen_value": gen_value, "gen_out": gen_out, "teacher_query": teacher_query, "teacher_key": teacher_key, "teacher_value": teacher_value, "teacher_out": teacher_out}


SHIFT = 5.0
EPS = 1e-06

def sigmas(steps, offset, count, total):
    level = 1.0 - steps.astype(jnp.float32) / STEPS
    sig = SHIFT * level / (1.0 + (SHIFT - 1.0) * level)
    positions = offset + jnp.arange(count, dtype=jnp.int32)
    frame = positions * FRAMES // total
    match = (frame[:, None] == jnp.arange(FRAMES, dtype=jnp.int32)[None, :]).astype(jnp.float32)
    return lax.optimization_barrier(jnp.sum(match * sig[None, :], axis=1))[:, None]

def normed(values):
    wide = values.astype(jnp.float32)
    return (wide * lax.rsqrt(lax.optimization_barrier(jnp.mean(wide * wide, axis=1, keepdims=True)) + EPS)).astype(jnp.bfloat16)

def attend(query, keys, values, allowed):
    scale = 1.0 / HEAD ** 0.5

    def single(head):
        start = head * HEAD
        q_head = lax.dynamic_slice_in_dim(query, start, HEAD, 1)
        k_head = lax.dynamic_slice_in_dim(keys, start, HEAD, 1)
        v_head = lax.dynamic_slice_in_dim(values, start, HEAD, 1)
        scores = jnp.dot(q_head, k_head.T, preferred_element_type=jnp.float32) * scale
        scores = jnp.where(allowed[None, :], scores, -1e+30)
        top = lax.optimization_barrier(jnp.max(scores, axis=1, keepdims=True))
        weights = jnp.where(allowed[None, :], jnp.exp(scores - top), 0.0)
        total = lax.optimization_barrier(jnp.sum(weights, axis=1, keepdims=True))
        return jnp.dot(weights.astype(jnp.bfloat16), v_head, preferred_element_type=jnp.float32) / total
    outputs = lax.map(single, jnp.arange(HEADS, dtype=jnp.int32))
    rows = query.shape[0]
    return jnp.transpose(outputs, (1, 0, 2)).reshape(rows, HEADS * HEAD).astype(jnp.bfloat16)

def grouped(attn, weight):
    width = HEADS * HEAD // N_FSDP

    def add(total, group):
        rows = lax.dynamic_slice_in_dim(attn, group * width, width, 1)
        cols = lax.dynamic_slice_in_dim(weight, group * width, width, 0)
        part = jnp.dot(rows, cols, preferred_element_type=jnp.float32)
        part = lax.optimization_barrier(part.astype(jnp.bfloat16)).astype(jnp.float32)
        return (total + part, None)
    start = jnp.zeros((attn.shape[0], weight.shape[1]), jnp.float32)
    total, _ = lax.scan(add, start, jnp.arange(N_FSDP, dtype=jnp.int32))
    return total

def reference(clean, noise, noise_two, steps_gen, steps_teacher, cache_key, cache_value, cache_block, span_block, gen_query, gen_key, gen_value, gen_out, teacher_query, teacher_key, teacher_value, teacher_out):
    total = clean.shape[0]
    sig_gen = sigmas(steps_gen, 0, total, total)
    sig_teacher = sigmas(steps_teacher, 0, total, total)
    mixed = ((1.0 - sig_gen) * clean.astype(jnp.float32) + sig_gen * noise.astype(jnp.float32)).astype(jnp.bfloat16)
    inputs = normed(mixed)
    query = jnp.dot(inputs, gen_query, preferred_element_type=jnp.float32).astype(jnp.bfloat16)
    key = jnp.dot(inputs, gen_key, preferred_element_type=jnp.float32).astype(jnp.bfloat16)
    value = jnp.dot(inputs, gen_value, preferred_element_type=jnp.float32).astype(jnp.bfloat16)
    allowed = jnp.concatenate([cache_block < span_block[0], jnp.ones((total,), bool)])
    attn = attend(query, jnp.concatenate([cache_key, key], 0), jnp.concatenate([cache_value, value], 0), allowed)
    generated = (mixed.astype(jnp.float32) + grouped(attn, gen_out)).astype(jnp.bfloat16)
    noisy = ((1.0 - sig_teacher) * generated.astype(jnp.float32) + sig_teacher * noise_two.astype(jnp.float32)).astype(jnp.bfloat16)
    inputs_two = normed(noisy)
    t_query = jnp.dot(inputs_two, teacher_query, preferred_element_type=jnp.float32).astype(jnp.bfloat16)
    t_key = jnp.dot(inputs_two, teacher_key, preferred_element_type=jnp.float32).astype(jnp.bfloat16)
    t_value = jnp.dot(inputs_two, teacher_value, preferred_element_type=jnp.float32).astype(jnp.bfloat16)
    teacher_attn = attend(t_query, t_key, t_value, jnp.ones((total,), bool))
    real = noisy.astype(jnp.float32) + grouped(teacher_attn, teacher_out)
    cotangent = (generated.astype(jnp.float32) - real).astype(jnp.bfloat16)
    grad_out = jnp.dot(attn.T, cotangent, preferred_element_type=jnp.float32).astype(jnp.bfloat16)
    return (generated, grad_out)
```

```python
import math

import jax
import jax.numpy as jnp
from jax import lax
from jax.experimental import pallas as pl
from jax.experimental.pallas import tpu as pltpu
from jax.sharding import Mesh
from jax.sharding import PartitionSpec as P

HEAD = 128
FRAMES = 3
STEPS = 1000
SHIFT = 5.0
EPS = 1e-06
CTX = ("yh", "z")
FSDP = ("x", "yl", "c")
BF = jnp.bfloat16
F32 = jnp.float32


def swap(x, axis):
    return lax.ppermute(x, axis, [(0, 1), (1, 0)])


def turn(x, axis, step):
    n = lax.axis_size(axis)
    return lax.ppermute(x, axis, [(i, (i + step) % n) for i in range(n)])


def sigmas(steps, offset, count, total):
    level = 1.0 - steps.astype(F32) / STEPS
    sig = SHIFT * level / (1.0 + (SHIFT - 1.0) * level)
    positions = offset + jnp.arange(count, dtype=jnp.int32)
    frame = positions * FRAMES // total
    match = (frame[:, None] == jnp.arange(FRAMES, dtype=jnp.int32)[None, :]).astype(F32)
    return jnp.sum(match * sig[None, :], axis=1)[:, None]


def normed(values):
    wide = values.astype(F32)
    return (wide * lax.rsqrt(jnp.mean(wide * wide, axis=1, keepdims=True) + EPS)).astype(BF)


def pick(flag, a, b):
    return jnp.where(flag, a, b)


def attend(queries, pieces, flags, offsets):
    rows = queries.shape[0]
    block = min(256, rows)
    sizes = [p.shape[0] for p in pieces]
    starts = [sum(sizes[:i]) for i in range(len(sizes))]
    masked = 0 if flags is None else flags.shape[0]
    factor = math.log2(math.e) / HEAD**0.5

    def body(*refs):
        q_ref = refs[0]
        refs = refs[1:]
        if masked:
            flag_ref = refs[0]
            refs = refs[1:]
        kv = refs[: len(pieces)]
        o_ref, s_ref = refs[len(pieces) :]
        q = q_ref[...]
        top = None
        for j, (r, off) in enumerate(zip(kv, offsets)):
            s = lax.dot_general(
                q, r[:, off : off + HEAD], (((1,), (1,)), ((), ())), preferred_element_type=F32
            )
            if j < masked:
                s = jnp.where(flag_ref[j : j + 1, :] > 0.0, s, -1e30)
            s_ref[:, starts[j] : starts[j] + sizes[j]] = s
            high = jnp.max(s, axis=1, keepdims=True)
            top = high if top is None else jnp.maximum(top, high)
        total = jnp.zeros((block, 1), F32)
        accum = jnp.zeros((block, HEAD), F32)
        for j, (r, off) in enumerate(zip(kv, offsets)):
            p = jnp.exp2((s_ref[:, starts[j] : starts[j] + sizes[j]] - top) * factor)
            total = total + jnp.sum(p, axis=1, keepdims=True)
            accum = accum + jnp.dot(
                p.astype(BF), r[:, off + HEAD : off + 2 * HEAD], preferred_element_type=F32
            )
        o_ref[...] = (accum / total).astype(BF)

    in_specs = [pl.BlockSpec((block, HEAD), lambda i: (i, 0))]
    args = [queries]
    if masked:
        in_specs.append(pl.BlockSpec(flags.shape, lambda i: (0, 0)))
        args.append(flags)
    for p in pieces:
        in_specs.append(pl.BlockSpec(p.shape, lambda i: (0, 0)))
        args.append(p)
    work = rows * sum(sizes) * HEAD
    return pl.pallas_call(
        body,
        grid=(rows // block,),
        in_specs=in_specs,
        out_specs=pl.BlockSpec((block, HEAD), lambda i: (i, 0)),
        out_shape=jax.ShapeDtypeStruct((rows, HEAD), BF),
        scratch_shapes=[pltpu.VMEM((block, sum(sizes)), F32)],
        compiler_params=pltpu.CompilerParams(vmem_limit_bytes=40 * 1024 * 1024),
        cost_estimate=pl.CostEstimate(
            flops=4 * work, transcendentals=rows * sum(sizes), bytes_accessed=4 * HEAD * sum(sizes)
        ),
    )(*args)


def project(rows, low, query_w, key_w, value_w):
    own = jnp.concatenate(
        [pick(low, w[:, :HEAD], w[:, HEAD:]) for w in (query_w, key_w, value_w)], axis=1
    )
    other = jnp.concatenate(
        [pick(low, w[:, HEAD:], w[:, :HEAD]) for w in (query_w, key_w, value_w)], axis=1
    )
    sent = jnp.dot(rows, other, preferred_element_type=F32).astype(BF)
    kept = jnp.dot(rows, own, preferred_element_type=F32).astype(BF)
    return kept, sent


def head_attention(kept, sent, cache, flags, low):
    recv = swap(sent, "yh")
    near = [turn(kept[:, HEAD:], "z", i) for i in (1, 2, 3)]
    far = [turn(recv[:, HEAD:], "z", i) for i in (1, 2, 3)]
    pieces = [*cache, kept, recv, *near, *far]
    offsets = [0] * len(cache) + [HEAD, HEAD] + [0] * 6
    theirs = attend(recv, pieces, flags, offsets)
    back = swap(theirs, "yh")
    mine = attend(kept, pieces, flags, offsets)
    return pick(
        low, jnp.concatenate([mine, back], axis=1), jnp.concatenate([back, mine], axis=1)
    )


def project_out(attn, weight):
    cores = lax.axis_size("c")
    x = lax.axis_index("x")
    y = lax.axis_index("yl")
    c = lax.axis_index("c")
    nx, ny = lax.axis_size("x"), lax.axis_size("yl")
    tok = attn.shape[0] // (nx * ny * cores)
    width = weight.shape[1]
    half = width // 2
    split = attn.reshape(nx * ny, cores, tok, attn.shape[1])
    first = split[:, 0].reshape(nx * ny * tok, -1)
    second = split[:, 1].reshape(nx * ny * tok, -1)
    sent = jnp.dot(pick(c == 0, second, first), weight, preferred_element_type=F32).astype(BF)
    recv = swap(sent, "c")
    kept = jnp.dot(pick(c == 0, first, second), weight, preferred_element_type=F32).astype(BF)
    chip = (kept.astype(F32) + recv.astype(F32)).astype(BF).reshape(nx, ny, tok, width)
    a = chip[..., :half]
    b = chip[..., half:]
    a_in = [
        turn(lax.dynamic_index_in_dim(a, (x + i) % nx, 0, keepdims=False), "x", i)
        for i in range(1, nx)
    ]
    b_in = swap(lax.dynamic_index_in_dim(b, 1 - y, 1, keepdims=False), "yl")
    a_sum = lax.dynamic_index_in_dim(a, x, 0, keepdims=False).astype(F32)
    for r in a_in:
        a_sum = a_sum + r.astype(F32)
    a_sum = a_sum.astype(BF)
    b_sum = (
        lax.dynamic_index_in_dim(b, y, 1, keepdims=False).astype(F32) + b_in.astype(F32)
    ).astype(BF)
    a_last = swap(lax.dynamic_index_in_dim(a_sum, 1 - y, 0, keepdims=False), "yl")
    b_last = [
        turn(lax.dynamic_index_in_dim(b_sum, (x + i) % nx, 0, keepdims=False), "x", i)
        for i in range(1, nx)
    ]
    a_all = lax.dynamic_index_in_dim(a_sum, y, 0, keepdims=False).astype(F32) + a_last.astype(F32)
    b_all = lax.dynamic_index_in_dim(b_sum, x, 0, keepdims=False).astype(F32)
    for r in b_last:
        b_all = b_all + r.astype(F32)
    return jnp.concatenate([a_all, b_all], axis=1)


def around_ctx(x):
    across = swap(x, "yh")
    near = [turn(x, "z", i) for i in (1, 2, 3)]
    far = [turn(across, "z", i) for i in (1, 2, 3)]
    return [x, *near, across, *far]


def place_columns(pieces, slots):
    rows, width = pieces[0].shape
    count = len(pieces)

    def body(slot_ref, *refs):
        for k in range(count):
            at = pl.multiple_of(slot_ref[k] * width, HEAD)
            refs[count][:, pl.ds(at, width)] = refs[k][...]

    return pl.pallas_call(
        body,
        in_specs=[pl.BlockSpec(memory_space=pltpu.SMEM)]
        + [pl.BlockSpec(memory_space=pltpu.VMEM)] * count,
        out_specs=pl.BlockSpec(memory_space=pltpu.VMEM),
        out_shape=jax.ShapeDtypeStruct((rows, width * count), pieces[0].dtype),
    )(slots, *pieces)


def gather_rows(x):
    return lax.all_gather(x, FSDP, axis=0, tiled=True)


def per_device(
    clean,
    noise,
    noise_two,
    steps_gen,
    steps_teacher,
    cache_key,
    cache_value,
    cache_block,
    span_block,
    gen_query,
    gen_key,
    gen_value,
    gen_out,
    teacher_query,
    teacher_key,
    teacher_value,
    teacher_out,
):
    ctx_count = lax.axis_size(CTX)
    fsdp_count = lax.axis_size(FSDP)
    tok_dev = clean.shape[0]
    total = tok_dev * fsdp_count * ctx_count
    width = clean.shape[1]
    offset = (lax.axis_index(CTX) * fsdp_count + lax.axis_index(FSDP)) * tok_dev
    low = lax.axis_index("yh") == 0
    z = lax.axis_index("z")
    nz = lax.axis_size("z")

    sig_gen = sigmas(steps_gen, offset, tok_dev, total)
    mixed = ((1.0 - sig_gen) * clean.astype(F32) + sig_gen * noise.astype(F32)).astype(BF)
    rows = gather_rows(normed(mixed))

    cache_own = jnp.concatenate(
        [pick(low, w[:, :HEAD], w[:, HEAD:]) for w in (cache_key, cache_value)], axis=1
    )
    cache_other = jnp.concatenate(
        [pick(low, w[:, HEAD:], w[:, :HEAD]) for w in (cache_key, cache_value)], axis=1
    )
    seen = (cache_block < span_block[0]).astype(F32)[None, :]
    cache_pair = jnp.concatenate([cache_own, swap(cache_other, "yh")], axis=0)
    seen_pair = jnp.concatenate([seen, swap(seen, "yh")], axis=1)
    cache = [cache_pair] + [turn(cache_pair, "z", i) for i in (1, 2, 3)]
    flags = jnp.concatenate([seen_pair] + [turn(seen_pair, "z", i) for i in (1, 2, 3)], axis=0)

    kept, sent = project(rows, low, gen_query, gen_key, gen_value)
    attn = head_attention(kept, sent, cache, flags, low)
    gen_sum = project_out(attn, gen_out)
    generated = (mixed.astype(F32) + gen_sum).astype(BF)
    sig_teacher = sigmas(steps_teacher, offset, tok_dev, total)
    noisy = (
        (1.0 - sig_teacher) * generated.astype(F32) + sig_teacher * noise_two.astype(F32)
    ).astype(BF)
    rows_two = gather_rows(normed(noisy))
    attn_all = around_ctx(attn)

    t_kept, t_sent = project(rows_two, low, teacher_query, teacher_key, teacher_value)
    teacher_attn = head_attention(t_kept, t_sent, [], None, low)
    real = noisy.astype(F32) + project_out(teacher_attn, teacher_out)
    cotangent = (generated.astype(F32) - real).astype(BF)

    part = width // ctx_count
    blocks = jnp.transpose(cotangent.reshape(tok_dev, 2, nz, part), (1, 2, 0, 3))
    yh = lax.axis_index("yh")
    same = lax.dynamic_index_in_dim(blocks, yh, 0, keepdims=False)
    other = swap(lax.dynamic_index_in_dim(blocks, 1 - yh, 0, keepdims=False), "yh")
    got = []
    for src in (same, other):
        got.append(lax.dynamic_index_in_dim(src, z, 0, keepdims=False))
        for i in (1, 2, 3):
            got.append(
                turn(lax.dynamic_index_in_dim(src, (z + i) % nz, 0, keepdims=False), "z", i)
            )
    mine = jnp.concatenate(got, axis=0)
    cot = gather_rows(mine)
    left = jnp.stack([a.reshape(fsdp_count, tok_dev, -1) for a in attn_all], axis=1)
    left = left.reshape(total, -1)
    slice_grad = lax.dot_general(
        left, cot, (((0,), (0,)), ((), ())), preferred_element_type=F32
    ).astype(BF)
    pieces = around_ctx(slice_grad)
    turns = (z - jnp.arange(nz, dtype=jnp.int32)) % nz
    slots = jnp.concatenate([yh * nz + turns, (1 - yh) * nz + turns]).astype(jnp.int32)
    grad_out = place_columns(pieces, slots)
    return (generated, grad_out)


def solution(mesh):
    fine = Mesh(mesh.devices.reshape(2, 4, 4, 2, 2), ("yh", "z", "x", "yl", "c"))
    tokens = P(CTX + FSDP, None)
    in_specs = (
        tokens,
        tokens,
        tokens,
        P(),
        P(),
        P(CTX, FSDP),
        P(CTX, FSDP),
        P(CTX),
        P(),
        P(None, FSDP),
        P(None, FSDP),
        P(None, FSDP),
        P(FSDP, None),
        P(None, FSDP),
        P(None, FSDP),
        P(None, FSDP),
        P(FSDP, None),
    )
    return jax.shard_map(
        per_device,
        mesh=fine,
        in_specs=in_specs,
        out_specs=(tokens, P(FSDP, None)),
        check_vma=False,
    )
```

```python
import math

import jax
import jax.numpy as jnp
from jax import lax
from jax.experimental import pallas as pl
from jax.experimental.pallas import tpu as pltpu
from jax.sharding import Mesh
from jax.sharding import PartitionSpec as P

HEAD = 128
FRAMES = 3
STEPS = 1000
SHIFT = 5.0
EPS = 1e-06
FLAG_ROWS = 16
CTX = ("yh", "z")
FSDP = ("x", "yl", "c")
BF = jnp.bfloat16
F32 = jnp.float32


def swap(x, axis):
    return lax.ppermute(x, axis, [(0, 1), (1, 0)])


def turn(x, axis, step):
    n = lax.axis_size(axis)
    return lax.ppermute(x, axis, [(i, (i + step) % n) for i in range(n)])


def sigmas(steps, offset, count, total):
    level = 1.0 - steps.astype(F32) / STEPS
    sig = SHIFT * level / (1.0 + (SHIFT - 1.0) * level)
    positions = offset + jnp.arange(count, dtype=jnp.int32)
    frame = positions * FRAMES // total
    match = (frame[:, None] == jnp.arange(FRAMES, dtype=jnp.int32)[None, :]).astype(F32)
    return jnp.sum(match * sig[None, :], axis=1)[:, None]


def normed(values):
    wide = values.astype(F32)
    return (wide * lax.rsqrt(jnp.mean(wide * wide, axis=1, keepdims=True) + EPS)).astype(BF)


def pick(flag, a, b):
    return jnp.where(flag, a, b)


def attend(queries, pieces):
    rows = queries.shape[0]
    block = min(256, rows)
    arrays = []
    for p in pieces:
        if all(p[0] is not q for q in arrays):
            arrays.append(p[0])
    where = [next(i for i, q in enumerate(arrays) if q is p[0]) for p in pieces]
    sizes = [p[2] for p in pieces]
    starts = [sum(sizes[:i]) for i in range(len(sizes))]
    plan = [(w, *p[1:], s) for w, p, s in zip(where, pieces, starts)]
    factor = math.log2(math.e) / HEAD**0.5

    def body(q_ref, *refs):
        o_ref, s_ref = refs[len(arrays) :]
        q = q_ref[...]
        top = None
        for w, row, size, col, flag, start in plan:
            keys = refs[w][row : row + size, col : col + HEAD]
            s = lax.dot_general(q, keys, (((1,), (1,)), ((), ())), preferred_element_type=F32)
            if flag is not None:
                s = jnp.where(refs[w][flag : flag + 1, :size].astype(F32) > 0.0, s, -1e30)
            s_ref[:, start : start + size] = s
            high = jnp.max(s, axis=1, keepdims=True)
            top = high if top is None else jnp.maximum(top, high)
        total = jnp.zeros((block, 1), F32)
        accum = jnp.zeros((block, HEAD), F32)
        for w, row, size, col, _, start in plan:
            p = jnp.exp2((s_ref[:, start : start + size] - top) * factor)
            total = total + jnp.sum(p, axis=1, keepdims=True)
            values = refs[w][row : row + size, col + HEAD : col + 2 * HEAD]
            accum = accum + jnp.dot(p.astype(BF), values, preferred_element_type=F32)
        o_ref[...] = (accum / total).astype(BF)

    work = rows * sum(sizes) * HEAD
    return pl.pallas_call(
        body,
        grid=(rows // block,),
        in_specs=[pl.BlockSpec((block, HEAD), lambda i: (i, 0))]
        + [pl.BlockSpec(a.shape, lambda i: (0, 0)) for a in arrays],
        out_specs=pl.BlockSpec((block, HEAD), lambda i: (i, 0)),
        out_shape=jax.ShapeDtypeStruct((rows, HEAD), BF),
        scratch_shapes=[pltpu.VMEM((block, sum(sizes)), F32)],
        compiler_params=pltpu.CompilerParams(vmem_limit_bytes=40 * 1024 * 1024),
        cost_estimate=pl.CostEstimate(
            flops=4 * work, transcendentals=rows * sum(sizes), bytes_accessed=4 * HEAD * sum(sizes)
        ),
    )(queries, *arrays)


def by_head(low, query_w, key_w, value_w):
    weights = (query_w, key_w, value_w)
    return jnp.concatenate(
        [pick(low, w[:, HEAD:], w[:, :HEAD]) for w in weights]
        + [pick(low, w[:, :HEAD], w[:, HEAD:]) for w in weights],
        axis=1,
    )


def project(rows, weights):
    across = swap(rows, "c")
    first = jnp.dot(rows, weights, preferred_element_type=F32).astype(BF)
    second = jnp.dot(across, weights, preferred_element_type=F32).astype(BF)
    width = 3 * HEAD
    sent = jnp.concatenate([first[:, :width], second[:, :width]], axis=0)
    kept = jnp.concatenate([first[:, width:], second[:, width:]], axis=0)
    return kept, sent


def head_attention(kept, sent, cache, low):
    recv = swap(sent, "yh")
    near = [turn(kept[:, HEAD:], "z", i) for i in (1, 3, 2)]
    far = [turn(recv[:, HEAD:], "z", i) for i in (1, 3, 2)]
    rows = kept.shape[0]
    pieces = []
    for c in cache:
        pair = c.shape[0] // 2
        slots = pair - FLAG_ROWS
        pieces += [(c, at, slots, 0, at + slots) for at in (0, pair)]
    pieces += [(p, 0, rows, HEAD, None) for p in (kept, recv)]
    pieces += [(p, 0, rows, 0, None) for p in (*near, *far)]
    theirs = attend(recv, pieces)
    back = swap(theirs, "yh")
    mine = attend(kept, pieces)
    return pick(
        low, jnp.concatenate([mine, back], axis=1), jnp.concatenate([back, mine], axis=1)
    )


def project_out(attn, weight):
    nx, ny = lax.axis_size("x"), lax.axis_size("yl")
    half_rows = attn.shape[0] // 2
    tok = half_rows // (nx * ny)
    half = weight.shape[1] // 2
    mine, theirs = attn[:half_rows], attn[half_rows:]
    parts = (weight[:, :half], weight[:, half:])
    sent = [jnp.dot(theirs, w, preferred_element_type=F32).astype(BF) for w in parts]
    recv = [swap(p, "c") for p in sent]
    kept = [jnp.dot(mine, w, preferred_element_type=F32).astype(BF) for w in parts]
    a, b = (
        (k.astype(F32) + r.astype(F32)).astype(BF).reshape(ny, nx, tok, half)
        for k, r in zip(kept, recv)
    )
    a_in = [turn(a[:, nx - i], "x", i) for i in (1, 3, 2)]
    b_in = swap(b[1], "yl")
    a_sum = a[:, 0].astype(F32)
    for r in a_in:
        a_sum = a_sum + r.astype(F32)
    a_sum = a_sum.astype(BF)
    b_sum = (b[0].astype(F32) + b_in.astype(F32)).astype(BF)
    a_last = swap(a_sum[1], "yl")
    b_last = [turn(b_sum[nx - i], "x", i) for i in (1, 3, 2)]
    a_all = a_sum[0].astype(F32) + a_last.astype(F32)
    b_all = b_sum[0].astype(F32)
    for r in b_last:
        b_all = b_all + r.astype(F32)
    return jnp.concatenate([a_all, b_all], axis=1)


def around_ctx(x):
    across = swap(x, "yh")
    near = [turn(x, "z", i) for i in (1, 2, 3)]
    far = [turn(across, "z", i) for i in (1, 2, 3)]
    return [x, *near, across, *far]


def place_columns(pieces, slots):
    rows, width = pieces[0].shape
    count = len(pieces)

    def body(slot_ref, *refs):
        for k in range(count):
            at = pl.multiple_of(slot_ref[k] * width, HEAD)
            refs[count][:, pl.ds(at, width)] = refs[k][...]

    return pl.pallas_call(
        body,
        in_specs=[pl.BlockSpec(memory_space=pltpu.SMEM)]
        + [pl.BlockSpec(memory_space=pltpu.VMEM)] * count,
        out_specs=pl.BlockSpec(memory_space=pltpu.VMEM),
        out_shape=jax.ShapeDtypeStruct((rows, width * count), pieces[0].dtype),
    )(slots, *pieces)


def chip_rows(x, cut):
    side = swap(x, "yl")
    row = [turn(x, "x", i) for i in (1, 3, 2)]
    row = [row[0], row[2], row[1]]
    low = [turn(side[cut:], "x", i) for i in (1, 3, 2)]
    low = [low[0], low[2], low[1]]
    high = [swap(r[:cut], "yl") for r in row]
    corner = [p for i in range(3) for p in (high[i], low[i])]
    return jnp.concatenate([x, *row, side, *corner], axis=0)


def per_device(
    clean,
    noise,
    noise_two,
    steps_gen,
    steps_teacher,
    cache_key,
    cache_value,
    cache_block,
    span_block,
    gen_query,
    gen_key,
    gen_value,
    gen_out,
    teacher_query,
    teacher_key,
    teacher_value,
    teacher_out,
):
    ctx_count = lax.axis_size(CTX)
    fsdp_count = lax.axis_size(FSDP)
    tok_dev = clean.shape[0]
    total = tok_dev * fsdp_count * ctx_count
    width = clean.shape[1]
    offset = (lax.axis_index(CTX) * fsdp_count + lax.axis_index(FSDP)) * tok_dev
    low = lax.axis_index("yh") == 0
    z = lax.axis_index("z")
    nz = lax.axis_size("z")

    sig_gen = sigmas(steps_gen, offset, tok_dev, total)
    mixed = ((1.0 - sig_gen) * clean.astype(F32) + sig_gen * noise.astype(F32)).astype(BF)
    rows = chip_rows(normed(mixed), tok_dev // 2)

    seen = (cache_block < span_block[0]).astype(BF)[None, :]
    seen = jnp.broadcast_to(seen, (FLAG_ROWS, seen.shape[1]))
    heads = (
        jnp.concatenate([w[:, :HEAD] for w in (cache_key, cache_value)], axis=1),
        jnp.concatenate([w[:, HEAD:] for w in (cache_key, cache_value)], axis=1),
    )
    cache_own = jnp.concatenate([pick(low, heads[0], heads[1]), seen], axis=0)
    cache_other = jnp.concatenate([pick(low, heads[1], heads[0]), seen], axis=0)
    cache_pair = jnp.concatenate([cache_own, swap(cache_other, "yh")], axis=0)
    cache = [cache_pair] + [turn(cache_pair, "z", i) for i in (1, 3, 2)]
    gen_weights = by_head(low, gen_query, gen_key, gen_value)
    teacher_weights = by_head(low, teacher_query, teacher_key, teacher_value)
    rows, cache, gen_weights, teacher_weights = lax.optimization_barrier(
        (rows, cache, gen_weights, teacher_weights)
    )

    kept, sent = project(rows, gen_weights)
    attn = head_attention(kept, sent, cache, low)
    attn_all = around_ctx(attn)
    gen_sum = project_out(attn, gen_out)
    generated = (mixed.astype(F32) + gen_sum).astype(BF)
    sig_teacher = sigmas(steps_teacher, offset, tok_dev, total)
    noisy = (
        (1.0 - sig_teacher) * generated.astype(F32) + sig_teacher * noise_two.astype(F32)
    ).astype(BF)
    rows_two = chip_rows(normed(noisy), tok_dev // 2)
    rows_two, attn_all = lax.optimization_barrier((rows_two, attn_all))
    t_kept, t_sent = project(rows_two, teacher_weights)
    teacher_attn = head_attention(t_kept, t_sent, [], low)
    real = noisy.astype(F32) + project_out(teacher_attn, teacher_out)
    cotangent = (generated.astype(F32) - real).astype(BF)

    part = width // ctx_count
    blocks = jnp.transpose(cotangent.reshape(tok_dev, 2, nz, part), (1, 2, 0, 3))
    yh = lax.axis_index("yh")
    same = lax.dynamic_index_in_dim(blocks, yh, 0, keepdims=False)
    other = swap(lax.dynamic_index_in_dim(blocks, 1 - yh, 0, keepdims=False), "yh")
    got = []
    for src in (same, other):
        got.append(lax.dynamic_index_in_dim(src, z, 0, keepdims=False))
        for i in (1, 2, 3):
            got.append(
                turn(lax.dynamic_index_in_dim(src, (z + i) % nz, 0, keepdims=False), "z", i)
            )
    mine = jnp.concatenate(got, axis=0)
    cot = chip_rows(mine, mine.shape[0] * 5 // 8)
    chips = fsdp_count // 2
    left = jnp.stack([a.reshape(2, chips, tok_dev, -1) for a in attn_all], axis=2)
    left = left.reshape(2, total // 2, -1)
    over = swap(cot, "c")
    first, second = (
        lax.dot_general(l, r, (((0,), (0,)), ((), ())), preferred_element_type=F32)
        for l, r in ((left[0], cot), (left[1], over))
    )
    slice_grad = (first + second).astype(BF)
    pieces = around_ctx(slice_grad)
    turns = (z - jnp.arange(nz, dtype=jnp.int32)) % nz
    slots = jnp.concatenate([yh * nz + turns, (1 - yh) * nz + turns]).astype(jnp.int32)
    grad_out = place_columns(pieces, slots)
    return (generated, grad_out)


def solution(mesh):
    fine = Mesh(mesh.devices.reshape(2, 4, 4, 2, 2), ("yh", "z", "x", "yl", "c"))
    tokens = P(CTX + FSDP, None)
    in_specs = (
        tokens,
        tokens,
        tokens,
        P(),
        P(),
        P(CTX, FSDP),
        P(CTX, FSDP),
        P(CTX),
        P(),
        P(None, FSDP),
        P(None, FSDP),
        P(None, FSDP),
        P(FSDP, None),
        P(None, FSDP),
        P(None, FSDP),
        P(None, FSDP),
        P(FSDP, None),
    )
    return jax.shard_map(
        per_device,
        mesh=fine,
        in_specs=in_specs,
        out_specs=(tokens, P(FSDP, None)),
        check_vma=False,
    )
```

```python
import math

import jax
import jax.numpy as jnp
from jax import lax
from jax.experimental import pallas as pl
from jax.experimental.pallas import tpu as pltpu
from jax.sharding import Mesh
from jax.sharding import PartitionSpec as P


HEAD = 128
FRAMES = 3
STEPS = 1000
SHIFT = 5.0
EPS = 1e-06
FLAG_ROWS = 16
CTX = ("yh", "z")
FSDP = ("x", "yl", "c")
BF = jnp.bfloat16
F32 = jnp.float32


def swap(x, axis):
    return lax.ppermute(x, axis, [(0, 1), (1, 0)])


def turn(x, axis, step):
    n = lax.axis_size(axis)
    return lax.ppermute(x, axis, [(i, (i + step) % n) for i in range(n)])


def sigmas(steps, offset, count, total):
    level = 1.0 - steps.astype(F32) / STEPS
    sig = SHIFT * level / (1.0 + (SHIFT - 1.0) * level)
    positions = offset + jnp.arange(count, dtype=jnp.int32)
    frame = positions * FRAMES // total
    match = (frame[:, None] == jnp.arange(FRAMES, dtype=jnp.int32)[None, :]).astype(F32)
    return jnp.sum(match * sig[None, :], axis=1)[:, None]


def normed(values):
    wide = values.astype(F32)
    return (wide * lax.rsqrt(jnp.mean(wide * wide, axis=1, keepdims=True) + EPS)).astype(BF)


def pick(flag, a, b):
    return jnp.where(flag, a, b)


def attend(queries, pieces, state=(), last=True):
    rows = queries.shape[0]
    block = min(256, rows)
    arrays = []
    for p in pieces:
        if all(p[0] is not q for q in arrays):
            arrays.append(p[0])
    where = [next(i for i, q in enumerate(arrays) if q is p[0]) for p in pieces]
    sizes = [p[2] for p in pieces]
    starts = [sum(sizes[:i]) for i in range(len(sizes))]
    plan = [(w, *p[1:], s) for w, p, s in zip(where, pieces, starts)]
    factor = math.log2(math.e) / HEAD**0.5

    def body(q_ref, *refs):
        before = refs[len(arrays) : len(arrays) + len(state)]
        outs, s_ref = refs[len(arrays) + len(state) : -1], refs[-1]
        q = q_ref[...]
        top = before[1][:, :1] if state else None
        for w, row, size, col, flag, start in plan:
            keys = refs[w][row : row + size, col : col + HEAD]
            s = lax.dot_general(q, keys, (((1,), (1,)), ((), ())), preferred_element_type=F32)
            if flag is not None:
                s = jnp.where(refs[w][flag : flag + 1, :size].astype(F32) > 0.0, s, -1e30)
            s_ref[:, start : start + size] = s
            high = jnp.max(s, axis=1, keepdims=True)
            top = high if top is None else jnp.maximum(top, high)
        if state:
            shrink = jnp.exp2((before[1][:, :1] - top) * factor)
            accum = before[0][...] * shrink
            total = before[2][:, :1] * shrink
        else:
            accum = jnp.zeros((block, HEAD), F32)
            total = jnp.zeros((block, 1), F32)
        for w, row, size, col, _, start in plan:
            p = jnp.exp2((s_ref[:, start : start + size] - top) * factor)
            total = total + jnp.sum(p, axis=1, keepdims=True)
            values = refs[w][row : row + size, col + HEAD : col + 2 * HEAD]
            accum = accum + jnp.dot(p.astype(BF), values, preferred_element_type=F32)
        if last:
            outs[0][...] = (accum / total).astype(BF)
        else:
            outs[0][...] = accum
            outs[1][...] = jnp.broadcast_to(top, (block, HEAD))
            outs[2][...] = jnp.broadcast_to(total, (block, HEAD))

    work = rows * sum(sizes) * HEAD
    tile = pl.BlockSpec((block, HEAD), lambda i: (i, 0))
    shape = (rows, HEAD)
    return pl.pallas_call(
        body,
        grid=(rows // block,),
        in_specs=[tile]
        + [pl.BlockSpec(a.shape, lambda i: (0, 0)) for a in arrays]
        + [tile] * len(state),
        out_specs=tile if last else [tile] * 3,
        out_shape=jax.ShapeDtypeStruct(shape, BF)
        if last
        else [jax.ShapeDtypeStruct(shape, F32)] * 3,
        scratch_shapes=[pltpu.VMEM((block, sum(sizes)), F32)],
        compiler_params=pltpu.CompilerParams(vmem_limit_bytes=40 * 1024 * 1024),
        cost_estimate=pl.CostEstimate(
            flops=4 * work, transcendentals=rows * sum(sizes), bytes_accessed=4 * HEAD * sum(sizes)
        ),
    )(queries, *arrays, *state)


def by_head(low, weights):
    return jnp.concatenate(
        [pick(low, w[:, :HEAD], w[:, HEAD:]) for w in weights]
        + [pick(low, w[:, HEAD:], w[:, :HEAD]) for w in weights],
        axis=1,
    )


def project(rows, weights):
    parts = [
        jnp.dot(r, weights, preferred_element_type=F32).astype(BF) for r in (rows, swap(rows, "c"))
    ]
    width = 3 * HEAD
    return (
        jnp.concatenate([p[:, :width] for p in parts], axis=0),
        jnp.concatenate([p[:, width:] for p in parts], axis=0),
    )


def head_attention(kept, sent, cache, low):
    recv = swap(sent, "yh")
    near = [turn(kept[:, HEAD:], "z", i) for i in (1, 3, 2)]
    far = [turn(recv[:, HEAD:], "z", i) for i in (1, 3, 2)]
    rows = kept.shape[0]
    pieces = []
    for c in cache:
        pair = c.shape[0] // 2
        slots = pair - FLAG_ROWS
        pieces += [(c, at, slots, 0, at + slots) for at in (0, pair)]
    pieces += [(p, 0, rows, HEAD, None) for p in (kept, recv)]
    pieces += [(p, 0, rows, 0, None) for p in near]
    their_state = attend(recv, pieces, last=False)
    my_state = attend(kept, pieces, last=False)
    far, their_state, my_state = lax.optimization_barrier((far, their_state, my_state))
    distant = [(p, 0, rows, 0, None) for p in far]
    theirs = attend(recv, distant, their_state)
    back = swap(theirs, "yh")
    mine = attend(kept, distant, my_state)
    return pick(
        low, jnp.concatenate([mine, back], axis=1), jnp.concatenate([back, mine], axis=1)
    )


def project_out(attn, weight):
    nx, ny = lax.axis_size("x"), lax.axis_size("yl")
    half_rows = attn.shape[0] // 2
    tok = half_rows // (nx * ny)
    half = weight.shape[1] // 2
    mine, theirs = attn[:half_rows], attn[half_rows:]
    parts = (weight[:, :half], weight[:, half:])
    sent = [jnp.dot(theirs, w, preferred_element_type=F32).astype(BF) for w in parts]
    recv = [swap(p, "c") for p in sent]
    kept = [jnp.dot(mine, w, preferred_element_type=F32).astype(BF) for w in parts]
    a, b = (
        (k.astype(F32) + r.astype(F32)).astype(BF).reshape(ny, nx, tok, half)
        for k, r in zip(kept, recv)
    )
    a_in = [turn(a[:, nx - i], "x", i) for i in (1, 3, 2)]
    b_in = swap(b[1], "yl")
    a_sum = a[:, 0].astype(F32)
    for r in a_in:
        a_sum = a_sum + r.astype(F32)
    a_sum = a_sum.astype(BF)
    b_sum = (b[0].astype(F32) + b_in.astype(F32)).astype(BF)
    a_last = swap(a_sum[1], "yl")
    b_last = [turn(b_sum[nx - i], "x", i) for i in (1, 3, 2)]
    a_all = a_sum[0].astype(F32) + a_last.astype(F32)
    b_all = b_sum[0].astype(F32)
    for r in b_last:
        b_all = b_all + r.astype(F32)
    return jnp.concatenate([a_all, b_all], axis=1)


def around_ctx(x):
    across = swap(x, "yh")
    near = [turn(x, "z", i) for i in (1, 2, 3)]
    far = [turn(across, "z", i) for i in (1, 2, 3)]
    return [x, *near, across, *far]


def place_columns(pieces, slots):
    rows, width = pieces[0].shape
    count = len(pieces)

    def body(slot_ref, *refs):
        for k in range(count):
            at = pl.multiple_of(slot_ref[k] * width, HEAD)
            refs[count][:, pl.ds(at, width)] = refs[k][...]

    return pl.pallas_call(
        body,
        in_specs=[pl.BlockSpec(memory_space=pltpu.SMEM)]
        + [pl.BlockSpec(memory_space=pltpu.VMEM)] * count,
        out_specs=pl.BlockSpec(memory_space=pltpu.VMEM),
        out_shape=jax.ShapeDtypeStruct((rows, width * count), pieces[0].dtype),
    )(slots, *pieces)


def chip_rows(x, cut):
    side = swap(x, "yl")
    row = [turn(x, "x", i) for i in (1, 3, 2)]
    row = [row[0], row[2], row[1]]
    low = [turn(side[cut:], "x", i) for i in (1, 3, 2)]
    low = [low[0], low[2], low[1]]
    high = [swap(r[:cut], "yl") for r in row]
    corner = [p for i in range(3) for p in (high[i], low[i])]
    return jnp.concatenate([x, *row, side, *corner], axis=0)


def per_device(
    clean,
    noise,
    noise_two,
    steps_gen,
    steps_teacher,
    cache_key,
    cache_value,
    cache_block,
    span_block,
    gen_query,
    gen_key,
    gen_value,
    gen_out,
    teacher_query,
    teacher_key,
    teacher_value,
    teacher_out,
):
    ctx_count = lax.axis_size(CTX)
    fsdp_count = lax.axis_size(FSDP)
    tok_dev = clean.shape[0]
    total = tok_dev * fsdp_count * ctx_count
    width = clean.shape[1]
    offset = (lax.axis_index(CTX) * fsdp_count + lax.axis_index(FSDP)) * tok_dev
    low = lax.axis_index("yh") == 0
    z = lax.axis_index("z")
    nz = lax.axis_size("z")

    sig_gen = sigmas(steps_gen, offset, tok_dev, total)
    mixed = ((1.0 - sig_gen) * clean.astype(F32) + sig_gen * noise.astype(F32)).astype(BF)
    seen = (cache_block < span_block[0]).astype(BF)[None, :]
    seen = jnp.broadcast_to(seen, (FLAG_ROWS, seen.shape[1]))
    heads = (
        jnp.concatenate([w[:, :HEAD] for w in (cache_key, cache_value)], axis=1),
        jnp.concatenate([w[:, HEAD:] for w in (cache_key, cache_value)], axis=1),
    )
    cache_own = jnp.concatenate([pick(low, heads[0], heads[1]), seen], axis=0)
    cache_other = jnp.concatenate([pick(low, heads[1], heads[0]), seen], axis=0)
    cache_pair = jnp.concatenate([cache_own, swap(cache_other, "yh")], axis=0)
    rows = chip_rows(normed(mixed), tok_dev // 2)
    cache = [cache_pair] + [turn(cache_pair, "z", i) for i in (1, 3, 2)]
    gen_weights = by_head(low, (gen_query, gen_key, gen_value))
    teacher_weights = by_head(low, (teacher_query, teacher_key, teacher_value))
    rows, cache, gen_weights, teacher_weights = lax.optimization_barrier(
        (rows, cache, gen_weights, teacher_weights)
    )

    kept, sent = project(rows, gen_weights)
    attn = head_attention(kept, sent, cache, low)
    across = swap(attn, "yh")
    attn_pair = jnp.concatenate([attn, across], axis=0)
    attn_all = [attn_pair] + [turn(attn_pair, "z", i) for i in (1, 2, 3)]
    gen_sum = project_out(attn, gen_out)
    generated = (mixed.astype(F32) + gen_sum).astype(BF)
    sig_teacher = sigmas(steps_teacher, offset, tok_dev, total)
    noisy = (
        (1.0 - sig_teacher) * generated.astype(F32) + sig_teacher * noise_two.astype(F32)
    ).astype(BF)
    rows_two = chip_rows(normed(noisy), tok_dev // 2)
    rows_two, attn_all = lax.optimization_barrier((rows_two, attn_all))
    t_kept, t_sent = project(rows_two, teacher_weights)
    teacher_attn = head_attention(t_kept, t_sent, [], low)
    real = noisy.astype(F32) + project_out(teacher_attn, teacher_out)
    cotangent = (generated.astype(F32) - real).astype(BF)

    part = width // ctx_count
    blocks = jnp.transpose(cotangent.reshape(tok_dev, 2, nz, part), (1, 2, 0, 3))
    yh = lax.axis_index("yh")
    same = lax.dynamic_index_in_dim(blocks, yh, 0, keepdims=False)
    other = swap(lax.dynamic_index_in_dim(blocks, 1 - yh, 0, keepdims=False), "yh")
    pair = jnp.stack([same, other], axis=1)
    got = [lax.dynamic_index_in_dim(pair, z, 0, keepdims=False)]
    for i in (1, 2, 3):
        got.append(turn(lax.dynamic_index_in_dim(pair, (z + i) % nz, 0, keepdims=False), "z", i))
    mine = jnp.stack(got, axis=0).reshape(ctx_count * tok_dev, part)
    cot = chip_rows(mine, mine.shape[0] * 5 // 8)
    chips = fsdp_count // 2
    left = jnp.stack([a.reshape(2, 2, chips, tok_dev, -1) for a in attn_all], axis=0)
    left = jnp.transpose(left, (2, 3, 0, 1, 4, 5)).reshape(2, total // 2, -1)
    over = swap(cot, "c")
    first, second = (
        lax.dot_general(l, r, (((0,), (0,)), ((), ())), preferred_element_type=F32)
        for l, r in ((left[0], cot), (left[1], over))
    )
    slice_grad = (first + second).astype(BF)
    pieces = around_ctx(slice_grad)
    turns = (z - jnp.arange(nz, dtype=jnp.int32)) % nz
    slots = jnp.concatenate([yh * nz + turns, (1 - yh) * nz + turns]).astype(jnp.int32)
    grad_out = place_columns(pieces, slots)
    return (generated, grad_out)


def solution(mesh):
    fine = Mesh(mesh.devices.reshape(2, 4, 4, 2, 2), ("yh", "z", "x", "yl", "c"))
    tokens = P(CTX + FSDP, None)
    in_specs = (
        tokens,
        tokens,
        tokens,
        P(),
        P(),
        P(CTX, FSDP),
        P(CTX, FSDP),
        P(CTX),
        P(),
        P(None, FSDP),
        P(None, FSDP),
        P(None, FSDP),
        P(FSDP, None),
        P(None, FSDP),
        P(None, FSDP),
        P(None, FSDP),
        P(FSDP, None),
    )

    return jax.shard_map(
        per_device,
        mesh=fine,
        in_specs=in_specs,
        out_specs=(tokens, P(FSDP, None)),
        check_vma=False,
    )
```
